32 devices in a mesh: data: 1 (over z), time: 32 (over y, x, core).
Axes of the slice: x: 4, y: 4, z: 1, core: 2. Of those that a mesh axis runs over, the one named last changes fastest.
The devices are a block of a 4x4x8 slice.
Arguments:
- x_init: float32 [4, 256, 1152], P('data')
- w_in: bfloat16 [1152, 4608], replicated
- w_out: bfloat16 [4608, 1152], replicated
- gamma_c: bfloat16 [64, 4608], P('time')
- beta_c: bfloat16 [64, 4608], P('time')
- gamma_u: bfloat16 [64, 4608], P('time')
- beta_u: bfloat16 [64, 4608], P('time')
- step_h: float32 [64], P('time')
- guide_w: float32 [1], replicated
Outputs:
- output: float32 [64, 4, 256, 1152], P('time', 'data')
All inputs are finite; a program needn't handle non-finite values.
Results may differ from the reference program's by a relative error of at most 0.00983.
Values are sent between devices in bfloat16 or wider.
A program may use at most 768 MiB of HBM per device.

```python
import jax
import jax.numpy as jnp
from jax import lax

SAMPLES = 4
TOKENS = 256
CHANNELS = 1152
HIDDEN = 4608
NUM_STEPS = 64
NUM_SWEEPS = 4


def setup_inputs(seed: int = 0, part: int = 0) -> dict:
    base_key = jax.random.key(seed)
    part_key = jax.random.fold_in(base_key, part)
    sub_keys = jax.random.split(base_key, 8)
    x_init = jax.random.normal(part_key, (SAMPLES, TOKENS, CHANNELS), jnp.float32)
    w_in = (jax.random.normal(sub_keys[0], (CHANNELS, HIDDEN), jnp.float32) * CHANNELS ** -0.5).astype(jnp.bfloat16)
    w_out = (jax.random.normal(sub_keys[1], (HIDDEN, CHANNELS), jnp.float32) * HIDDEN ** -0.5).astype(jnp.bfloat16)
    gamma_c = (0.5 * jax.random.normal(sub_keys[2], (NUM_STEPS, HIDDEN), jnp.float32)).astype(jnp.bfloat16)
    beta_c = (0.5 * jax.random.normal(sub_keys[3], (NUM_STEPS, HIDDEN), jnp.float32)).astype(jnp.bfloat16)
    gamma_u = (0.5 * jax.random.normal(sub_keys[4], (NUM_STEPS, HIDDEN), jnp.float32)).astype(jnp.bfloat16)
    beta_u = (0.5 * jax.random.normal(sub_keys[5], (NUM_STEPS, HIDDEN), jnp.float32)).astype(jnp.bfloat16)
    step_h = jax.random.normal(sub_keys[6], (NUM_STEPS,), jnp.float32) * (0.6 * NUM_STEPS ** -0.5)
    guide_w = jax.random.uniform(sub_keys[7], (1,), jnp.float32, 1.0, 3.0)
    return {"x_init": x_init, "w_in": w_in, "w_out": w_out, "gamma_c": gamma_c, "beta_c": beta_c, "gamma_u": gamma_u, "beta_u": beta_u, "step_h": step_h, "guide_w": guide_w}


def reference(x_init, w_in, w_out, gamma_c, beta_c, gamma_u, beta_u, step_h, guide_w):
    guide = guide_w[0]
    tok_rows = SAMPLES * TOKENS

    def one_step(step_args):
        x_step, cond_gain, cond_shift, unc_gain, unc_shift, h_one = step_args
        pre_act = jnp.dot(x_step.reshape(tok_rows, CHANNELS).astype(jnp.bfloat16), w_in, preferred_element_type=jnp.float32)
        act_c = jax.nn.gelu(pre_act * (1.0 + cond_gain.astype(jnp.float32)) + cond_shift.astype(jnp.float32)).astype(jnp.bfloat16)
        act_u = jax.nn.gelu(pre_act * (1.0 + unc_gain.astype(jnp.float32)) + unc_shift.astype(jnp.float32)).astype(jnp.bfloat16)
        out_c = jnp.dot(act_c, w_out, preferred_element_type=jnp.float32)
        out_u = jnp.dot(act_u, w_out, preferred_element_type=jnp.float32)
        drift = h_one * ((1.0 + guide) * out_c - guide * out_u)
        return drift.reshape(SAMPLES, TOKENS, CHANNELS)

    def sweep(states, unused):
        drifts = lax.map(one_step, (states, gamma_c, beta_c, gamma_u, beta_u, step_h))
        earlier = jnp.cumsum(drifts[:-1], axis=0)
        offsets = jnp.concatenate([jnp.zeros_like(drifts[:1]), earlier], axis=0)
        return x_init[None] + offsets, None

    start = jnp.broadcast_to(x_init[None], (NUM_STEPS, SAMPLES, TOKENS, CHANNELS))
    final, ignored = lax.scan(sweep, start, None, length=NUM_SWEEPS)
    return final
```

```python
import jax
import jax.numpy as jnp
from jax import lax
from jax.sharding import PartitionSpec as P

NUM_SWEEPS = 4


def solution(mesh):
    num_time = mesh.shape["time"]

    def local(x_init, w_in, w_out, gamma_c, beta_c, gamma_u, beta_u, step_h, guide_w):
        samples, tokens, channels = x_init.shape
        own_steps, hidden = gamma_c.shape
        steps = own_steps * num_time
        total_rows = samples * tokens
        rows = total_rows // num_time
        guide = guide_w[0]

        mods = jnp.stack([gamma_c, beta_c, gamma_u, beta_u], axis=1)
        mods = lax.all_gather(mods, "time", axis=0, tiled=True).astype(jnp.float32)
        gains = (1.0 + mods[:, 0], 1.0 + mods[:, 2])
        shifts = (mods[:, 1], mods[:, 3])
        h_all = lax.all_gather(step_h, "time", axis=0, tiled=True)

        me = lax.axis_index("time")
        x_rows = lax.dynamic_slice_in_dim(x_init.reshape(total_rows, channels), me * rows, rows, axis=0)

        def drift(states, lo, hi):
            pre = jnp.einsum("krc,cd->krd", states.astype(jnp.bfloat16), w_in, preferred_element_type=jnp.float32)
            outs = []
            for gain, shift in zip(gains, shifts):
                act = jax.nn.gelu(pre * gain[lo:hi, None, :] + shift[lo:hi, None, :]).astype(jnp.bfloat16)
                outs.append(jnp.einsum("krd,dc->krc", act, w_out, preferred_element_type=jnp.float32))
            return h_all[lo:hi, None, None] * ((1.0 + guide) * outs[0] - guide * outs[1])

        drifts = drift(x_rows[None], 0, steps - 1)
        for index in range(1, NUM_SWEEPS):
            running = jnp.cumsum(drifts, axis=0)
            states = x_rows[None] + running[index - 1:steps - 2]
            drifts = jnp.concatenate([drifts[:index], drift(states, index, steps - 1)], axis=0)
        running = jnp.cumsum(drifts, axis=0)
        final = jnp.concatenate([x_rows[None], x_rows[None] + running], axis=0)
        final = lax.all_to_all(final, "time", split_axis=0, concat_axis=1, tiled=True)
        return final.reshape(own_steps, samples, tokens, channels)

    return jax.shard_map(local, mesh=mesh, in_specs=(P("data", None, None), P(None, None), P(None, None), P("time", None), P("time", None), P("time", None), P("time", None), P("time"), P(None)), out_specs=P("time", "data", None, None), check_vma=False)
```

```python
import functools
import math

import jax
import jax.numpy as jnp
from jax import lax
from jax.experimental import pallas as pl
from jax.experimental.pallas import tpu as pltpu
from jax.sharding import PartitionSpec as P

NUM_SWEEPS = 4
ROWS = 8
TILE = 256
MESH = pl.DeviceIdType.MESH
LIN = 2.0 * math.sqrt(2.0 / math.pi)
CUB = 8.0 * 0.044715 * math.sqrt(2.0 / math.pi)


def kernel(num_time, chunk, x_hbm, w_in_hbm, w_out_hbm, mods_hbm, h_ref, guide_ref, land, x_v, w_in, w_out, mods, a0, act, acc, xb, f0, out_v, load_sem, send_sem, self_sem, recv_sem):
    me = lax.axis_index("time")
    steps = mods.shape[1]
    own = steps // num_time
    rows, channels = x_v.shape
    hidden = w_in.shape[1]
    groups = rows // ROWS
    inner = steps - 2

    barrier = pltpu.get_barrier_semaphore()

    def signal(i, carry):
        pl.semaphore_signal(barrier, inc=1, device_id={"time": lax.rem(me + i, num_time)}, device_id_type=MESH)
        return carry

    lax.fori_loop(1, num_time, signal, 0)

    def load(src, dst, sem, parts):
        size = dst.shape[0] // parts
        for i in range(parts):
            pltpu.make_async_copy(src.at[pl.ds(i * size, size)], dst.at[pl.ds(i * size, size)], sem).start()

    load(x_hbm.at[pl.ds(me * rows, rows)], x_v, load_sem.at[0], 1)
    load(w_in_hbm, w_in, load_sem.at[1], 8)
    load(mods_hbm, mods, load_sem.at[2], 4)
    load(w_out_hbm, w_out, load_sem.at[3], 8)

    def loaded(dst, sem):
        pltpu.make_async_copy(dst, dst, sem).wait()

    gain_c, gain_u = 1.0 + guide_ref[0], guide_ref[0]

    def clear(j, carry):
        acc[pl.ds(pl.multiple_of(j * ROWS, ROWS), ROWS), :] = jnp.zeros((ROWS, channels), jnp.float32)
        return carry

    lax.fori_loop(0, steps, clear, 0)

    loaded(x_v, load_sem.at[0])
    loaded(w_in, load_sem.at[1])
    x_cast = x_v[...].astype(jnp.bfloat16)

    def first_act(t, carry):
        cols = pl.ds(pl.multiple_of(t * TILE, TILE), TILE)
        a0[:, cols] = jnp.dot(x_cast, w_in[:, cols], preferred_element_type=jnp.float32)
        return carry

    lax.fori_loop(0, hidden // TILE, first_act, 0)
    loaded(mods, load_sem.at[2])
    loaded(w_out, load_sem.at[3])
    pl.semaphore_wait(barrier, num_time - 1)

    def gelu(z):
        return z + z * jnp.tanh(z * (LIN + CUB * (z * z)))

    def activate(pre_of, lo, count, col, sub):
        cols = pl.ds(col, TILE)
        for pair in range(count // 2):
            for e in range(2):
                halves = []
                for q in range(2):
                    j = lo + 2 * pair + q
                    gain = mods[2 * e, pl.ds(j, 1), cols]
                    shift = mods[2 * e + 1, pl.ds(j, 1), cols]
                    halves.append(gelu(pre_of(2 * pair + q) * gain + shift))
                act[e, pl.ds(2 * ROWS * pair, 2 * ROWS), pl.ds(sub * TILE, TILE)] = jnp.concatenate(halves, axis=0).astype(jnp.bfloat16)

    def project(t, lo, count):
        deep = pl.ds(pl.multiple_of(t * chunk, TILE), chunk)
        for n0 in range(0, channels, TILE):
            wide = pl.ds(n0, min(TILE, channels - n0))
            weights = w_out[deep, wide]
            cond = jnp.dot(act[0, pl.ds(0, count * ROWS), :], weights, preferred_element_type=jnp.float32)
            unc = jnp.dot(act[1, pl.ds(0, count * ROWS), :], weights, preferred_element_type=jnp.float32)
            acc[pl.ds(lo * ROWS, count * ROWS), wide] += gain_c * cond - gain_u * unc

    def take_drift(j):
        where = pl.ds(j * ROWS, ROWS)
        drift = h_ref[j] * acc[where, :]
        acc[where, :] = jnp.zeros((ROWS, channels), jnp.float32)
        return drift

    def to_states(x_g):
        total = f0[...]
        for pair in range(inner // 2):
            first = x_g + total
            total = total + take_drift(1 + 2 * pair)
            second = x_g + total
            total = total + take_drift(2 + 2 * pair)
            xb[pl.ds(2 * ROWS * pair, 2 * ROWS), :] = jnp.concatenate([first, second], axis=0).astype(jnp.bfloat16)

    def to_output(x_g, slot):
        out_v[slot, 0] = x_g
        total = f0[...]
        for j in range(1, steps):
            out_v[slot, j] = x_g + total
            if j < steps - 1:
                total = total + take_drift(j)

    def sent_wait(slot):
        pltpu.make_async_copy(out_v.at[slot, pl.ds(0, steps - own)], out_v.at[slot, pl.ds(0, steps - own)], send_sem.at[slot]).wait()
        pltpu.make_async_copy(out_v.at[slot, pl.ds(0, own)], out_v.at[slot, pl.ds(0, own)], self_sem.at[slot]).wait()

    def group(g, carry):
        mine = pl.ds(pl.multiple_of(g * ROWS, ROWS), ROWS)
        slot = lax.rem(g, 2)
        x_g = x_v[mine, :]

        def first_chunk(t, c):
            for sub in range(chunk // TILE):
                col = pl.multiple_of(t * chunk + sub * TILE, TILE)
                pre = a0[mine, pl.ds(col, TILE)]
                activate(lambda i, pre=pre: pre, 0, steps, col, sub)
            project(t, 0, steps)
            return c

        lax.fori_loop(0, hidden // chunk, first_chunk, 0)
        f0[...] = take_drift(0)
        to_states(x_g)

        def sweep(k, c):
            def one_chunk(t, c2):
                for sub in range(chunk // TILE):
                    col = pl.multiple_of(t * chunk + sub * TILE, TILE)
                    pre = jnp.dot(xb[...], w_in[:, pl.ds(col, TILE)], preferred_element_type=jnp.float32)
                    activate(lambda i, pre=pre: pre[i * ROWS:(i + 1) * ROWS, :], 1, inner, col, sub)
                project(t, 1, inner)
                return c2

            lax.fori_loop(0, hidden // chunk, one_chunk, 0)

            @pl.when(k < NUM_SWEEPS - 1)
            def _():
                to_states(x_g)

            @pl.when(k == NUM_SWEEPS - 1)
            def _():
                @pl.when(g >= 2)
                def _():
                    sent_wait(slot)

                to_output(x_g, slot)

            return c

        lax.fori_loop(1, NUM_SWEEPS, sweep, 0)

        acc[pl.ds((steps - 1) * ROWS, ROWS), :] = jnp.zeros((ROWS, channels), jnp.float32)

        there = pl.ds(pl.multiple_of(me * rows + g * ROWS, ROWS), ROWS)
        pltpu.make_async_copy(out_v.at[slot, pl.ds(me * own, own)], land.at[:, there, :], self_sem.at[slot]).start()

        def send(i, c):
            dest = lax.rem(me + i, num_time)
            pltpu.make_async_remote_copy(
                src_ref=out_v.at[slot, pl.ds(dest * own, own)],
                dst_ref=land.at[:, there, :],
                send_sem=send_sem.at[slot],
                recv_sem=recv_sem.at[0],
                device_id={"time": dest},
                device_id_type=MESH,
            ).start()
            return c

        lax.fori_loop(1, num_time, send, 0)
        return carry

    lax.fori_loop(0, groups, group, 0)
    for slot in range(min(2, groups)):
        sent_wait(slot)
    arrived = land.at[:, pl.ds(0, land.shape[1] - rows), :]
    pltpu.make_async_copy(arrived, arrived, recv_sem.at[0]).wait()


def solution(mesh):
    num_time = mesh.shape["time"]

    def local(x_init, w_in, w_out, gamma_c, beta_c, gamma_u, beta_u, step_h, guide_w):
        samples, tokens, channels = x_init.shape
        own, hidden = gamma_c.shape
        steps = own * num_time
        total_rows = samples * tokens
        rows = total_rows // num_time
        chunk = hidden // 3 if hidden % (3 * TILE) == 0 else hidden // 2

        mods = jnp.stack([gamma_c, beta_c, gamma_u, beta_u], axis=1)
        mods = lax.all_gather(mods, "time", axis=0, tiled=True).astype(jnp.float32)
        one = jnp.asarray([1.0, 0.0, 1.0, 0.0], jnp.float32)
        mods = jnp.swapaxes(0.5 * (mods + one[None, :, None]), 0, 1)
        h_all = lax.all_gather(step_h, "time", axis=0, tiled=True)

        hbm = pl.BlockSpec(memory_space=pl.ANY)
        smem = pl.BlockSpec(memory_space=pltpu.SMEM)
        f32, bf16 = jnp.float32, jnp.bfloat16
        out = pl.pallas_call(
            functools.partial(kernel, num_time, chunk),
            out_shape=jax.ShapeDtypeStruct((own, total_rows, channels), f32),
            in_specs=[hbm, hbm, hbm, hbm, smem, smem],
            out_specs=hbm,
            scratch_shapes=[
                pltpu.VMEM((rows, channels), f32),
                pltpu.VMEM((channels, hidden), bf16),
                pltpu.VMEM((hidden, channels), bf16),
                pltpu.VMEM((4, steps, hidden), f32),
                pltpu.VMEM((rows, hidden), f32),
                pltpu.VMEM((2, steps * ROWS, chunk), bf16),
                pltpu.VMEM((steps * ROWS, channels), f32),
                pltpu.VMEM(((steps - 2) * ROWS, channels), bf16),
                pltpu.VMEM((ROWS, channels), f32),
                pltpu.VMEM((2, steps, ROWS, channels), f32),
                pltpu.SemaphoreType.DMA((4,)),
                pltpu.SemaphoreType.DMA((2,)),
                pltpu.SemaphoreType.DMA((2,)),
                pltpu.SemaphoreType.DMA((1,)),
            ],
            compiler_params=pltpu.CompilerParams(collective_id=0, has_side_effects=True, vmem_limit_bytes=63 * 1024 * 1024),
        )(x_init.reshape(total_rows, channels), w_in, w_out, mods, h_all, guide_w)
        return out.reshape(own, samples, tokens, channels)

    return jax.shard_map(local, mesh=mesh, in_specs=(P("data", None, None), P(None, None), P(None, None), P("time", None), P("time", None), P("time", None), P("time", None), P("time"), P(None)), out_specs=P("time", "data", None, None), check_vma=False)
```

```python
import functools
import math

import jax
import jax.numpy as jnp
from jax import lax
from jax.experimental import pallas as pl
from jax.experimental.pallas import tpu as pltpu
from jax.sharding import PartitionSpec as P

NUM_SWEEPS = 4
ROWS = 8
TILE = 256
MESH = pl.DeviceIdType.MESH
LIN = 2.0 * math.sqrt(2.0 / math.pi)
CUB = 8.0 * 0.044715 * math.sqrt(2.0 / math.pi)


def kernel(num_time, chunk, x_hbm, w_in_hbm, w_out_hbm, mods_src, h_src, guide_ref, land, x_v, w_in, w_out, gathered, mods, h_all, a0, act, acc, xb, f0, out_v, load_sem, give_sem, take_sem, send_sem, self_sem, recv_sem):
    me = lax.axis_index("time")
    own = h_src.shape[0]
    steps = own * num_time
    rows, channels = x_v.shape
    hidden = w_in.shape[1]
    groups = rows // ROWS
    num_chunks = hidden // chunk
    inner = steps - 2
    stride = 7 if math.gcd(7 * 15, num_time) == 1 else 1

    barrier = pltpu.get_barrier_semaphore()

    def signal(i, carry):
        pl.semaphore_signal(barrier, inc=1, device_id={"time": lax.rem(me + i, num_time)}, device_id_type=MESH)
        return carry

    lax.fori_loop(1, num_time, signal, 0)

    def to_peers(send):
        def one(i, carry):
            dest = lax.rem(me + stride * (i + 2 * me), num_time)

            @pl.when(dest != me)
            def _():
                send(dest)

            return carry

        lax.fori_loop(0, num_time, one, 0)

    def remote(src, dst, send, recv, dest):
        return pltpu.make_async_remote_copy(src_ref=src, dst_ref=dst, send_sem=send, recv_sem=recv, device_id={"time": dest}, device_id_type=MESH)

    def load(src, dst, sem, parts):
        size = dst.shape[0] // parts
        for i in range(parts):
            pltpu.make_async_copy(src.at[pl.ds(i * size, size)], dst.at[pl.ds(i * size, size)], sem).start()

    def settle(ref, sem):
        pltpu.make_async_copy(ref, ref, sem).wait()

    load(x_hbm.at[pl.ds(me * rows, rows)], x_v, load_sem.at[0], 1)
    load(w_in_hbm, w_in, load_sem.at[1], 8)
    load(w_out_hbm, w_out, load_sem.at[2], 8)

    pl.semaphore_wait(barrier, num_time - 1)
    for t in range(num_chunks):
        to_peers(lambda dest, t=t: remote(mods_src.at[t], gathered.at[t, me], give_sem.at[0], take_sem.at[t], dest).start())
    to_peers(lambda dest: remote(h_src, h_all.at[me], give_sem.at[1], take_sem.at[num_chunks], dest).start())
    for t in range(num_chunks):
        gathered[t, me] = mods_src[t]
    h_all[me] = h_src[...]

    gain_c, gain_u = 1.0 + guide_ref[0], guide_ref[0]

    def clear(j, carry):
        for g in range(groups):
            acc[g, pl.ds(pl.multiple_of(j * ROWS, ROWS), ROWS), :] = jnp.zeros((ROWS, channels), jnp.float32)
        return carry

    lax.fori_loop(0, steps, clear, 0)

    settle(x_v, load_sem.at[0])
    settle(w_in, load_sem.at[1])
    x_cast = x_v[...].astype(jnp.bfloat16)

    def first_act(t, carry):
        cols = pl.ds(pl.multiple_of(t * 2 * TILE, 2 * TILE), 2 * TILE)
        a0[:, cols] = jnp.dot(x_cast, w_in[:, cols], preferred_element_type=jnp.float32)
        return carry

    lax.fori_loop(0, hidden // (2 * TILE), first_act, 0)
    settle(w_out, load_sem.at[2])

    def gelu(z):
        return z + z * jnp.tanh(z * (LIN + CUB * (z * z)))

    def activate(pre_of, lo, count, col, sub):
        cols = pl.ds(col, TILE)
        for pair in range(count // 2):
            for e in range(2):
                halves = []
                for q in range(2):
                    j = lo + 2 * pair + q
                    gain = mods[j // own, pl.ds(2 * e * own + j % own, 1), cols]
                    shift = mods[j // own, pl.ds((2 * e + 1) * own + j % own, 1), cols]
                    halves.append(gelu(pre_of(2 * pair + q) * gain + shift))
                act[e, pl.ds(2 * ROWS * pair, 2 * ROWS), pl.ds(sub * TILE, TILE)] = jnp.concatenate(halves, axis=0).astype(jnp.bfloat16)

    def project(g, t, lo, count):
        deep = pl.ds(pl.multiple_of(t * chunk, TILE), chunk)
        for n0 in range(0, channels, TILE):
            wide = pl.ds(n0, min(TILE, channels - n0))
            weights = w_out[deep, wide]
            cond = jnp.dot(act[0, pl.ds(0, count * ROWS), :], weights, preferred_element_type=jnp.float32)
            unc = jnp.dot(act[1, pl.ds(0, count * ROWS), :], weights, preferred_element_type=jnp.float32)
            acc[g, pl.ds(lo * ROWS, count * ROWS), wide] += gain_c * cond - gain_u * unc

    def take_drift(g, j):
        where = pl.ds(j * ROWS, ROWS)
        h = jnp.concatenate([h_all[j // own, j % own]] * (channels // 128), axis=1)
        drift = h * acc[g, where, :]
        acc[g, where, :] = jnp.zeros((ROWS, channels), jnp.float32)
        return drift

    def to_states(g, x_g):
        total = f0[...]
        for pair in range(inner // 2):
            first = x_g + total
            total = total + take_drift(g, 1 + 2 * pair)
            second = x_g + total
            total = total + take_drift(g, 2 + 2 * pair)
            xb[pl.ds(2 * ROWS * pair, 2 * ROWS), :] = jnp.concatenate([first, second], axis=0).astype(jnp.bfloat16)

    def to_output(g, x_g, slot):
        out_v[slot, 0] = x_g
        total = f0[...]
        for j in range(1, steps):
            out_v[slot, j] = x_g + total
            if j < steps - 1:
                total = total + take_drift(g, j)

    def sent_wait(slot):
        settle(out_v.at[slot, pl.ds(0, steps - own)], send_sem.at[slot])
        settle(out_v.at[slot, pl.ds(0, own)], self_sem.at[slot])

    row_kind = lax.broadcasted_iota(jnp.int32, (4 * own, chunk), 0) // own
    half = jnp.where(row_kind % 2 == 0, 0.5, 0.0).astype(jnp.float32)

    def first_chunk(t, carry):
        settle(gathered.at[t, pl.ds(0, num_time - 1)], take_sem.at[t])

        def widen(d, c):
            mods[d, :, pl.ds(pl.multiple_of(t * chunk, TILE), chunk)] = 0.5 * gathered[t, d].astype(jnp.float32) + half
            return c

        lax.fori_loop(0, num_time, widen, 0)

        def first_group(g, c):
            for sub in range(chunk // TILE):
                col = pl.multiple_of(t * chunk + sub * TILE, TILE)
                pre = a0[pl.ds(pl.multiple_of(g * ROWS, ROWS), ROWS), pl.ds(col, TILE)]
                activate(lambda i, pre=pre: pre, 0, steps, col, sub)
            project(g, t, 0, steps)
            return c

        lax.fori_loop(0, groups, first_group, 0)
        return carry

    lax.fori_loop(0, num_chunks, first_chunk, 0)
    settle(h_all.at[pl.ds(0, num_time - 1)], take_sem.at[num_chunks])

    def group(g, carry):
        slot = lax.rem(g, 2)
        x_g = x_v[pl.ds(pl.multiple_of(g * ROWS, ROWS), ROWS), :]
        f0[...] = take_drift(g, 0)
        to_states(g, x_g)

        def sweep(k, c):
            def one_chunk(t, c2):
                for sub in range(chunk // TILE):
                    col = pl.multiple_of(t * chunk + sub * TILE, TILE)
                    pre = jnp.dot(xb[...], w_in[:, pl.ds(col, TILE)], preferred_element_type=jnp.float32)
                    activate(lambda i, pre=pre: pre[i * ROWS:(i + 1) * ROWS, :], 1, inner, col, sub)
                project(g, t, 1, inner)
                return c2

            lax.fori_loop(0, num_chunks, one_chunk, 0)

            @pl.when(k < NUM_SWEEPS - 1)
            def _():
                to_states(g, x_g)

            @pl.when(k == NUM_SWEEPS - 1)
            def _():
                @pl.when(g >= 2)
                def _():
                    sent_wait(slot)

                to_output(g, x_g, slot)

            return c

        lax.fori_loop(1, NUM_SWEEPS, sweep, 0)

        there = pl.ds(pl.multiple_of(me * rows + g * ROWS, ROWS), ROWS)
        pltpu.make_async_copy(out_v.at[slot, pl.ds(me * own, own)], land.at[:, there, :], self_sem.at[slot]).start()
        to_peers(lambda dest: remote(out_v.at[slot, pl.ds(dest * own, own)], land.at[:, there, :], send_sem.at[slot], recv_sem.at[0], dest).start())
        return carry

    lax.fori_loop(0, groups, group, 0)
    settle(gathered.at[:, pl.ds(0, num_time - 1)], give_sem.at[0])
    settle(h_all.at[pl.ds(0, num_time - 1)], give_sem.at[1])
    for slot in range(min(2, groups)):
        sent_wait(slot)
    settle(land.at[:, pl.ds(0, land.shape[1] - rows), :], recv_sem.at[0])


def solution(mesh):
    num_time = mesh.shape["time"]

    def local(x_init, w_in, w_out, gamma_c, beta_c, gamma_u, beta_u, step_h, guide_w):
        samples, tokens, channels = x_init.shape
        own, hidden = gamma_c.shape
        steps = own * num_time
        total_rows = samples * tokens
        rows = total_rows // num_time
        chunk = hidden // 3 if hidden % (3 * TILE) == 0 else hidden // 2

        num_chunks = hidden // chunk
        mods = jnp.stack([gamma_c, beta_c, gamma_u, beta_u], axis=0).reshape(4 * own, num_chunks, chunk)
        mods = jnp.swapaxes(mods, 0, 1)
        h_wide = jnp.broadcast_to(step_h[:, None, None], (own, ROWS, 128))

        hbm = pl.BlockSpec(memory_space=pl.ANY)
        vmem = pl.BlockSpec(memory_space=pltpu.VMEM)
        smem = pl.BlockSpec(memory_space=pltpu.SMEM)
        f32, bf16 = jnp.float32, jnp.bfloat16
        out = pl.pallas_call(
            functools.partial(kernel, num_time, chunk),
            out_shape=jax.ShapeDtypeStruct((own, total_rows, channels), f32),
            in_specs=[hbm, hbm, hbm, vmem, vmem, smem],
            out_specs=hbm,
            scratch_shapes=[
                pltpu.VMEM((rows, channels), f32),
                pltpu.VMEM((channels, hidden), bf16),
                pltpu.VMEM((hidden, channels), bf16),
                pltpu.VMEM((num_chunks, num_time, 4 * own, chunk), bf16),
                pltpu.VMEM((num_time, 4 * own, hidden), f32),
                pltpu.VMEM((num_time, own, ROWS, 128), f32),
                pltpu.VMEM((rows, hidden), f32),
                pltpu.VMEM((2, steps * ROWS, chunk), bf16),
                pltpu.VMEM((rows // ROWS, steps * ROWS, channels), f32),
                pltpu.VMEM(((steps - 2) * ROWS, channels), bf16),
                pltpu.VMEM((ROWS, channels), f32),
                pltpu.VMEM((2, steps, ROWS, channels), f32),
                pltpu.SemaphoreType.DMA((3,)),
                pltpu.SemaphoreType.DMA((2,)),
                pltpu.SemaphoreType.DMA((num_chunks + 1,)),
                pltpu.SemaphoreType.DMA((2,)),
                pltpu.SemaphoreType.DMA((2,)),
                pltpu.SemaphoreType.DMA((1,)),
            ],
            compiler_params=pltpu.CompilerParams(collective_id=0, has_side_effects=True, vmem_limit_bytes=63 * 1024 * 1024),
        )(x_init.reshape(total_rows, channels), w_in, w_out, mods, h_wide, guide_w)
        return out.reshape(own, samples, tokens, channels)

    return jax.shard_map(local, mesh=mesh, in_specs=(P("data", None, None), P(None, None), P(None, None), P("time", None), P("time", None), P("time", None), P("time", None), P("time"), P(None)), out_specs=P("time", "data", None, None), check_vma=False)
```

```python
import functools
import math

import jax
import jax.numpy as jnp
from jax import lax
from jax.experimental import pallas as pl
from jax.experimental.pallas import tpu as pltpu
from jax.sharding import PartitionSpec as P

NUM_SWEEPS = 4
ROWS = 8
TILE = 256
MESH = pl.DeviceIdType.MESH
LIN = 2.0 * math.sqrt(2.0 / math.pi)
CUB = 8.0 * 0.044715 * math.sqrt(2.0 / math.pi)


def kernel(num_time, chunk, x_hbm, w_in_hbm, w_out_hbm, mods_src, h_src, guide_ref, land, x_v, w_in, w_out, gathered, mods, h_all, a0, act, acc, xb, f0, out_v, load_sem, give_sem, take_sem, send_sem, self_sem, recv_sem):
    me = lax.axis_index("time")
    own = h_src.shape[0]
    steps = own * num_time
    rows, channels = x_v.shape
    hidden = w_in.shape[1]
    groups = rows // ROWS
    num_chunks = hidden // chunk
    inner = steps - 2
    stride = 7 if math.gcd(7 * 15, num_time) == 1 else 1

    barrier = pltpu.get_barrier_semaphore()

    def signal(i, carry):
        pl.semaphore_signal(barrier, inc=1, device_id={"time": lax.rem(me + i, num_time)}, device_id_type=MESH)
        return carry

    lax.fori_loop(1, num_time, signal, 0)

    def to_peers(send):
        def one(i, carry):
            dest = lax.rem(me + stride * (i + 2 * me), num_time)

            @pl.when(dest != me)
            def _():
                send(dest)

            return carry

        lax.fori_loop(0, num_time, one, 0)

    def remote(src, dst, send, recv, dest):
        return pltpu.make_async_remote_copy(src_ref=src, dst_ref=dst, send_sem=send, recv_sem=recv, device_id={"time": dest}, device_id_type=MESH)

    def load(src, dst, sem, parts):
        size = dst.shape[0] // parts
        for i in range(parts):
            pltpu.make_async_copy(src.at[pl.ds(i * size, size)], dst.at[pl.ds(i * size, size)], sem).start()

    def settle(ref, sem):
        pltpu.make_async_copy(ref, ref, sem).wait()

    load(x_hbm.at[pl.ds(me * rows, rows)], x_v, load_sem.at[0], 1)
    load(w_in_hbm, w_in, load_sem.at[1], 8)
    load(w_out_hbm, w_out, load_sem.at[2], 8)

    pl.semaphore_wait(barrier, num_time - 1)
    for t in range(num_chunks):
        to_peers(lambda dest, t=t: remote(mods_src.at[t], gathered.at[t, me], give_sem.at[0], take_sem.at[t], dest).start())
    to_peers(lambda dest: remote(h_src, h_all.at[me], give_sem.at[1], take_sem.at[num_chunks], dest).start())
    for t in range(num_chunks):
        gathered[t, me] = mods_src[t]
    h_all[me] = h_src[...]

    gain_c, gain_u = 1.0 + guide_ref[0], guide_ref[0]

    def clear(j, carry):
        for g in range(groups):
            acc[g, pl.ds(pl.multiple_of(j * ROWS, ROWS), ROWS), :] = jnp.zeros((ROWS, channels), jnp.float32)
        return carry

    lax.fori_loop(0, steps, clear, 0)

    settle(x_v, load_sem.at[0])
    settle(w_in, load_sem.at[1])
    x_cast = x_v[...].astype(jnp.bfloat16)

    def first_act(t, carry):
        cols = pl.ds(pl.multiple_of(t * 2 * TILE, 2 * TILE), 2 * TILE)
        a0[:, cols] = jnp.dot(x_cast, w_in[:, cols], preferred_element_type=jnp.float32)
        return carry

    lax.fori_loop(0, hidden // (2 * TILE), first_act, 0)
    settle(w_out, load_sem.at[2])

    def gelu(z):
        return z + z * jnp.tanh(z * (LIN + CUB * (z * z)))

    def activate(pre_of, lo, count, col, sub):
        cols = pl.ds(col, TILE)
        for pair in range(count // 2):
            for e in range(2):
                halves = []
                for q in range(2):
                    j = lo + 2 * pair + q
                    block = mods[j // own, :, cols]
                    gain = block[2 * e * own + j % own:2 * e * own + j % own + 1, :]
                    at = (2 * e + 1) * own + j % own
                    halves.append(gelu(pre_of(2 * pair + q) * gain + block[at:at + 1, :]))
                act[e, pl.ds(2 * ROWS * pair, 2 * ROWS), pl.ds(sub * TILE, TILE)] = jnp.concatenate(halves, axis=0).astype(jnp.bfloat16)

    def project(g, t, lo, count):
        deep = pl.ds(pl.multiple_of(t * chunk, TILE), chunk)
        for n0 in range(0, channels, TILE):
            wide = pl.ds(n0, min(TILE, channels - n0))
            weights = w_out[deep, wide]
            cond = jnp.dot(act[0, pl.ds(0, count * ROWS), :], weights, preferred_element_type=jnp.float32)
            unc = jnp.dot(act[1, pl.ds(0, count * ROWS), :], weights, preferred_element_type=jnp.float32)
            acc[g, pl.ds(lo * ROWS, count * ROWS), wide] += gain_c * cond - gain_u * unc

    def take_drift(g, j):
        where = pl.ds(j * ROWS, ROWS)
        h = jnp.concatenate([h_all[j // own, j % own]] * (channels // 128), axis=1)
        drift = h * acc[g, where, :]
        acc[g, where, :] = jnp.zeros((ROWS, channels), jnp.float32)
        return drift

    def to_states(g, x_g):
        total = f0[...]
        for pair in range(inner // 2):
            first = x_g + total
            total = total + take_drift(g, 1 + 2 * pair)
            second = x_g + total
            total = total + take_drift(g, 2 + 2 * pair)
            xb[pl.ds(2 * ROWS * pair, 2 * ROWS), :] = jnp.concatenate([first, second], axis=0).astype(jnp.bfloat16)

    def to_output(g, x_g, slot):
        out_v[slot, 0] = x_g
        total = f0[...]
        for j in range(1, steps):
            out_v[slot, j] = x_g + total
            if j < steps - 1:
                total = total + take_drift(g, j)

    def sent_wait(slot):
        settle(out_v.at[slot, pl.ds(0, steps - own)], send_sem.at[slot])
        settle(out_v.at[slot, pl.ds(0, own)], self_sem.at[slot])

    row_kind = lax.broadcasted_iota(jnp.int32, (4 * own, chunk), 0) // own
    half = jnp.where(row_kind % 2 == 0, 0.5, 0.0).astype(jnp.float32)

    def first_chunk(t, carry):
        settle(gathered.at[t, pl.ds(0, num_time - 1)], take_sem.at[t])

        def widen(d, c):
            mods[d, :, pl.ds(pl.multiple_of(t * chunk, TILE), chunk)] = 0.5 * gathered[t, d].astype(jnp.float32) + half
            return c

        lax.fori_loop(0, num_time, widen, 0)

        def first_group(g, c):
            for sub in range(chunk // TILE):
                col = pl.multiple_of(t * chunk + sub * TILE, TILE)
                pre = a0[pl.ds(pl.multiple_of(g * ROWS, ROWS), ROWS), pl.ds(col, TILE)]
                activate(lambda i, pre=pre: pre, 0, steps, col, sub)
            project(g, t, 0, steps)
            return c

        lax.fori_loop(0, groups, first_group, 0)
        return carry

    lax.fori_loop(0, num_chunks, first_chunk, 0)
    settle(h_all.at[pl.ds(0, num_time - 1)], take_sem.at[num_chunks])

    def group(g, carry):
        slot = lax.rem(g, 2)
        x_g = x_v[pl.ds(pl.multiple_of(g * ROWS, ROWS), ROWS), :]
        f0[...] = take_drift(g, 0)
        to_states(g, x_g)

        def sweep(k, c):
            def one_chunk(t, c2):
                for sub in range(chunk // TILE):
                    col = pl.multiple_of(t * chunk + sub * TILE, TILE)
                    pre = jnp.dot(xb[...], w_in[:, pl.ds(col, TILE)], preferred_element_type=jnp.float32)
                    activate(lambda i, pre=pre: pre[i * ROWS:(i + 1) * ROWS, :], 1, inner, col, sub)
                project(g, t, 1, inner)
                return c2

            lax.fori_loop(0, num_chunks, one_chunk, 0)

            @pl.when(k < NUM_SWEEPS - 1)
            def _():
                to_states(g, x_g)

            @pl.when(k == NUM_SWEEPS - 1)
            def _():
                @pl.when(g >= 2)
                def _():
                    sent_wait(slot)

                to_output(g, x_g, slot)

            return c

        lax.fori_loop(1, NUM_SWEEPS, sweep, 0)

        there = pl.ds(pl.multiple_of(me * rows + g * ROWS, ROWS), ROWS)
        pltpu.make_async_copy(out_v.at[slot, pl.ds(me * own, own)], land.at[:, there, :], self_sem.at[slot]).start()
        to_peers(lambda dest: remote(out_v.at[slot, pl.ds(dest * own, own)], land.at[:, there, :], send_sem.at[slot], recv_sem.at[0], dest).start())
        return carry

    lax.fori_loop(0, groups, group, 0)
    settle(gathered.at[:, pl.ds(0, num_time - 1)], give_sem.at[0])
    settle(h_all.at[pl.ds(0, num_time - 1)], give_sem.at[1])
    for slot in range(min(2, groups)):
        sent_wait(slot)
    settle(land.at[:, pl.ds(0, land.shape[1] - rows), :], recv_sem.at[0])


def solution(mesh):
    num_time = mesh.shape["time"]

    def local(x_init, w_in, w_out, gamma_c, beta_c, gamma_u, beta_u, step_h, guide_w):
        samples, tokens, channels = x_init.shape
        own, hidden = gamma_c.shape
        steps = own * num_time
        total_rows = samples * tokens
        rows = total_rows // num_time
        chunk = hidden // 3 if hidden % (3 * TILE) == 0 else hidden // 2

        num_chunks = hidden // chunk
        mods = jnp.stack([gamma_c, beta_c, gamma_u, beta_u], axis=0).reshape(4 * own, num_chunks, chunk)
        mods = jnp.swapaxes(mods, 0, 1)
        h_wide = jnp.broadcast_to(step_h[:, None, None], (own, ROWS, 128))

        hbm = pl.BlockSpec(memory_space=pl.ANY)
        vmem = pl.BlockSpec(memory_space=pltpu.VMEM)
        smem = pl.BlockSpec(memory_space=pltpu.SMEM)
        f32, bf16 = jnp.float32, jnp.bfloat16
        out = pl.pallas_call(
            functools.partial(kernel, num_time, chunk),
            out_shape=jax.ShapeDtypeStruct((own, total_rows, channels), f32),
            in_specs=[hbm, hbm, hbm, vmem, vmem, smem],
            out_specs=hbm,
            scratch_shapes=[
                pltpu.VMEM((rows, channels), f32),
                pltpu.VMEM((channels, hidden), bf16),
                pltpu.VMEM((hidden, channels), bf16),
                pltpu.VMEM((num_chunks, num_time, 4 * own, chunk), bf16),
                pltpu.VMEM((num_time, 4 * own, hidden), f32),
                pltpu.VMEM((num_time, own, ROWS, 128), f32),
                pltpu.VMEM((rows, hidden), f32),
                pltpu.VMEM((2, steps * ROWS, chunk), bf16),
                pltpu.VMEM((rows // ROWS, steps * ROWS, channels), f32),
                pltpu.VMEM(((steps - 2) * ROWS, channels), bf16),
                pltpu.VMEM((ROWS, channels), f32),
                pltpu.VMEM((2, steps, ROWS, channels), f32),
                pltpu.SemaphoreType.DMA((3,)),
                pltpu.SemaphoreType.DMA((2,)),
                pltpu.SemaphoreType.DMA((num_chunks + 1,)),
                pltpu.SemaphoreType.DMA((2,)),
                pltpu.SemaphoreType.DMA((2,)),
                pltpu.SemaphoreType.DMA((1,)),
            ],
            compiler_params=pltpu.CompilerParams(collective_id=0, has_side_effects=True, vmem_limit_bytes=63 * 1024 * 1024),
        )(x_init.reshape(total_rows, channels), w_in, w_out, mods, h_wide, guide_w)
        return out.reshape(own, samples, tokens, channels)

    return jax.shard_map(local, mesh=mesh, in_specs=(P("data", None, None), P(None, None), P(None, None), P("time", None), P("time", None), P("time", None), P("time", None), P("time"), P(None)), out_specs=P("time", "data", None, None), check_vma=False)
```
